256 devices in a mesh: section: 4 (over x), mesh: 64 (over z, y, core).
Axes of the slice: x: 4, y: 4, z: 8, core: 2. Of those that a mesh axis runs over, the one named last changes fastest.
Arguments:
- video_tokens: bfloat16 [2, 128, 6144], P(None, 'mesh'), may hold values from -6 to 6
- norm_gain: float32 [4, 6144], P('section'), may hold values from 0.5 to 2
- qkv_weight: bfloat16 [4, 6144, 18432], P('section', None, 'mesh'), may hold values from -0.078125 to 0.078125
- out_weight: bfloat16 [4, 6144, 6144], P('section', 'mesh'), may hold values from -0.078125 to 0.078125
Outputs:
- final_tokens: float32 [2, 128, 6144], P(None, 'mesh', 'section')
The draws below stay inside these ranges and needn't reach their ends.
All inputs are finite; a program needn't handle non-finite values.
Results may differ from the reference program's by a relative error of at most 0.023.
Values may be sent and summed in bfloat16 or wider, within the bound.
A program may use at most 64 MiB of HBM per device.

```python
import jax
import jax.numpy as jnp
from jax import lax

D = 6144
HEADS = 64
HEAD_DIM = 96
PATCHES = 64
FRAMES = 2
MICRO = 2
SECTIONS = 4
TOKENS = 128


def draw_norm_gain(key, part):
    return jax.random.uniform(key, (SECTIONS, D), jnp.float32, 0.6, 1.6)


def block_levels(rng, dims, cuts, least, high):
    gain = 1.0
    for dim, shards_of in cuts:
        steps = jax.random.uniform(jax.random.fold_in(jax.random.fold_in(rng, 6), dim), (shards_of,), jnp.float32, least / len(cuts), high / len(cuts))
        gain = gain * jnp.repeat(jnp.exp(steps), dims[dim] // shards_of).reshape((-1,) + (1,) * (len(dims) - 1 - dim))
    return gain


def scatter_about(stream_key, shape, deviation, bound, split=(), held_as=jnp.bfloat16):
    result = jax.random.normal(stream_key, shape, jnp.float32) * deviation
    if len(split) > 0:
        result = block_levels(stream_key, shape, split, -0.22, 0.18) * result
    return jnp.clip(result, min=-bound, max=bound).astype(held_as)


def setup_inputs(seed: int = 0) -> dict:
    key_list = jax.random.split(jax.random.key(seed), 5)
    video_tokens = scatter_about(key_list[0], (MICRO, TOKENS, D), 1.0, 6.0, ((1, 64),))
    norm_gain = draw_norm_gain(jax.random.fold_in(key_list[4], 71), 0)
    qkv_weight = scatter_about(key_list[2], (SECTIONS, D, 3 * HEADS * HEAD_DIM), D ** -0.5, 0.078125, ((0, 4), (2, 64)))
    out_weight = scatter_about(key_list[3], (SECTIONS, HEADS * HEAD_DIM, D), (HEADS * HEAD_DIM) ** -0.5, 0.078125, ((0, 4), (1, 64)))
    return {"video_tokens": video_tokens, "norm_gain": norm_gain, "qkv_weight": qkv_weight, "out_weight": out_weight}


epsilon = 1e-06

def token_masks():
    row_ids = jnp.arange(FRAMES * PATCHES, dtype=jnp.int32)
    same_frame = row_ids[:, None] // PATCHES == row_ids[None, :] // PATCHES
    same_patch = row_ids[:, None] % PATCHES == row_ids[None, :] % PATCHES
    return (same_frame, same_patch)

def attention_layer(residual, gain_row, packed_weight, out_rows, attend_mask):
    wide = residual.astype(jnp.float32)
    mean_square = lax.optimization_barrier(jnp.mean(wide * wide, axis=-1, keepdims=True))
    normed = (wide * lax.rsqrt(mean_square + epsilon) * gain_row[None, :].astype(jnp.float32)).astype(jnp.bfloat16)
    packed = jnp.dot(normed, packed_weight, preferred_element_type=jnp.float32).astype(jnp.bfloat16)
    tokens = normed.shape[0]
    packed = packed.reshape(tokens, HEADS, 3, HEAD_DIM)
    queries = packed[:, :, 0].astype(jnp.float32)
    key_rows = packed[:, :, 1].astype(jnp.float32)
    value_rows = packed[:, :, 2].astype(jnp.float32)
    scores = jnp.einsum('thd,shd->hts', queries, key_rows) * HEAD_DIM ** (-0.5)
    scores = jnp.where(attend_mask[None], scores, -1e+30)
    weights = jax.nn.softmax(scores, axis=-1).astype(jnp.bfloat16)
    attended = jnp.einsum('hts,shd->thd', weights.astype(jnp.float32), value_rows)
    attended = attended.astype(jnp.bfloat16).reshape(tokens, HEADS * HEAD_DIM)
    projected = jnp.dot(attended, out_rows, preferred_element_type=jnp.float32)
    return wide + projected

def reference(video_tokens, norm_gain, qkv_weight, out_weight):
    same_frame, same_patch = token_masks()
    results = []
    for micro in range(MICRO):
        residual = video_tokens[micro].astype(jnp.float32)
        for layer in range(SECTIONS):
            attend_mask = same_frame if layer % 2 == 0 else same_patch
            residual = attention_layer(residual, norm_gain[layer], qkv_weight[layer], out_weight[layer], attend_mask)
        results.append(residual)
    return jnp.stack(results)
```

```python
import jax
import jax.numpy as jnp
from jax import lax
from jax.experimental import pallas as pl
from jax.experimental.pallas import tpu as pltpu
from jax.sharding import PartitionSpec as P

MESH = pl.DeviceIdType.MESH
HEAD = 96
PAD = 128
Z, Y, G = 8, 4, 8
ROWS = 16
WIDE = 768
TOKENS = 128
D = 6144
LAST = 3
EPS = 1e-06
ORDER = (0, 1, 7, 2, 6, 3, 5, 4)
BF = jnp.bfloat16
F32 = jnp.float32


def kernel(
    tok_ref, gain_ref, w_hbm, wo_hbm, out_ref,
    x, wraw, wp, wo, acc, ssq, att, part, rsb, slab, fin, ini_s, ini_r,
    wsem, ini_ss, ini_rs, wo_ss, wo_rs, wo_ls, zi_ss, z_ss, z_rs, y_ss, y_rs, r_ss, r_rs,
    d_ss, d_rs, a_ss, a_rs, p_ss, p_rs, f_ss, f_rs,
):
    s = lax.axis_index("section")
    me = lax.axis_index("mesh")
    z, j = me // G, me % G
    y, c = j // 2, j % 2

    def at(sec, zz, jj):
        return (sec, zz * G + jj)

    def send(src, dst, ssem, rsem, dev):
        pltpu.make_async_remote_copy(
            src_ref=src, dst_ref=dst, send_sem=ssem, recv_sem=rsem, device_id=dev, device_id_type=MESH
        ).start()

    def drain(ref, sem):
        pltpu.make_async_copy(ref, ref, sem).wait()

    def rows(zz):
        return pl.ds(pl.multiple_of(zz * ROWS, ROWS), ROWS)

    def other(jj, k):
        return (jj + k) % G

    wcopy = pltpu.make_async_copy(w_hbm, wraw, wsem)
    wcopy.start()
    own_wo = pltpu.make_async_copy(
        wo_hbm.at[:, pl.ds(pl.multiple_of(j * WIDE, WIDE), WIDE)], wo.at[j, pl.ds(0, HEAD)], wo_ls
    )
    own_wo.start()

    barrier = pltpu.get_barrier_semaphore()

    def greet(dev):
        pl.semaphore_signal(barrier, inc=1, device_id=dev, device_id_type=MESH)

    for k in range(1, G):
        greet(at(s, z, other(j, k)))
    for k in range(1, Z):
        greet(at(s, (z + k) % Z, j))

    @pl.when(s < LAST)
    def _():
        for k in range(Z):
            greet(at(s + 1, k, j))
        for k in range(2):
            greet(at(LAST, z, 2 * s + k))

    @pl.when(s > 0)
    def _():
        for k in range(Z):
            greet(at(s - 1, k, j))

    @pl.when(jnp.logical_and(s == LAST, y < LAST))
    def _():
        for k in range(G):
            greet(at(y, z, k))

    greeted = G - 1 + Z - 1 + jnp.where(s < LAST, Z + 2, 0) + jnp.where(s > 0, Z, 0)
    pl.semaphore_wait(barrier, greeted + jnp.where(jnp.logical_and(s == LAST, y < LAST), G, 0))

    @pl.when(s == 0)
    def _():
        for g in range(G):
            for m in range(2):
                ini_s[g, m] = tok_ref[m, :, g * WIDE:(g + 1) * WIDE].astype(F32)
        for k in range(1, G):
            to = other(j, k)
            send(ini_s.at[to], ini_r.at[j], ini_ss, ini_rs, at(s, z, to))

    for k in range(1, G):
        to = other(j, k)
        send(
            wo_hbm.at[:, pl.ds(pl.multiple_of(to * WIDE, WIDE), WIDE)], wo.at[j, pl.ds(0, HEAD)],
            wo_ss, wo_rs, at(s, z, to),
        )
    for g in range(G):
        wo[g, HEAD:PAD, :] = jnp.zeros((PAD - HEAD, WIDE), BF)

    wcopy.wait()

    def prepare(g, carry):
        for i in range(WIDE // 128):
            at_row = pl.multiple_of(g * WIDE + i * 128, 128)
            gain = jnp.broadcast_to(gain_ref[:, pl.ds(at_row, 128)], (128, 128)).T[:, :HEAD]
            w = wraw[pl.ds(at_row, 128), :].astype(F32)
            blank = jnp.zeros((128, PAD - HEAD), F32)
            for q in range(3):
                piece = w[:, q * HEAD:(q + 1) * HEAD] * gain
                wp[g, i * 128:(i + 1) * 128, q * PAD:(q + 1) * PAD] = jnp.concatenate([piece, blank], axis=1).astype(BF)
        return carry

    lax.fori_loop(0, G, prepare, 0)

    def spread(src, m, sec, ssem, skip_own):
        for d in ORDER:
            if d == 0 and skip_own:
                continue
            send(src, x.at[m, j, rows(z)], ssem, z_rs.at[m, z], at(sec, (z + d) % Z, j))

    @pl.when(s == 0)
    def _():
        ini_r[j] = ini_s[j]
        drain(ini_r.at[pl.ds(0, G - 1)], ini_rs)
        for m in range(2):
            whole = jnp.concatenate([ini_r[g, m] for g in range(G)], axis=0).astype(BF)
            slab[m] = whole
            x[m, j, rows(z), :] = whole
            spread(slab.at[m], m, s, zi_ss.at[m], True)

    def take_rows(m):
        for i, d in enumerate(ORDER):
            zz = (z + d) % Z
            chunk = x.at[m, j, rows(zz)]
            if d == 0:
                @pl.when(s > 0)
                def _():
                    drain(chunk, z_rs.at[m, zz])
            else:
                drain(chunk, z_rs.at[m, zz])
            half = 0 if i < 4 else 1
            send(chunk, chunk, y_ss.at[m], y_rs.at[m, 0, half], at(s, z, other(j, 2)))
            send(chunk, chunk, y_ss.at[m], y_rs.at[m, 1, half], at(s, z, other(j, 6)))
        share(m, 0, j)

    def sibling(jj):
        return jj + 1 - 2 * c

    def share(m, slot, jj):
        send(x.at[m, jj], x.at[m, jj], d_ss.at[m], d_rs.at[m, slot], at(s, z, sibling(j)))

    def multiply(m, jj, first=False):
        xs = x[m, jj]
        wide = xs.astype(F32)
        squares = wide * wide
        total = squares[:, :128]
        for i in range(1, WIDE // 128):
            total += squares[:, i * 128:(i + 1) * 128]
        product = jnp.dot(xs, wp[jj], preferred_element_type=F32)
        if first:
            acc[m] = product
            ssq[m] = total
        else:
            acc[m] += product
            ssq[m] += total

    def relay(m, jj, half, to, slot):
        for d in ORDER[half * 4:half * 4 + 4]:
            chunk = x.at[m, jj, rows((z + d) % Z)]
            send(chunk, chunk, r_ss.at[m], r_rs.at[m, slot], at(s, z, to))

    def take_groups(m):
        before, after, across = other(j, 6), other(j, 2), other(j, 4)
        half_rows = pl.ds(0, TOKENS // 2)
        multiply(m, j, True)
        drain(x.at[m, before, half_rows], y_rs.at[m, 0, 0])
        relay(m, before, 0, after, 0)
        drain(x.at[m, after, half_rows], y_rs.at[m, 1, 0])
        drain(x.at[m, after, half_rows], y_rs.at[m, 1, 1])
        relay(m, after, 1, before, 1)
        share(m, 1, after)
        drain(x.at[m, before, half_rows], y_rs.at[m, 0, 1])
        share(m, 2, before)
        multiply(m, after)
        multiply(m, before)
        drain(x.at[m, j], d_rs.at[m, 0])
        multiply(m, sibling(j))
        drain(x.at[m, across, half_rows], r_rs.at[m, 0])
        drain(x.at[m, across, half_rows], r_rs.at[m, 1])
        share(m, 3, across)
        multiply(m, across)
        for slot, jj in ((1, after), (2, before), (3, across)):
            drain(x.at[m, jj], d_rs.at[m, slot])
            multiply(m, sibling(jj))

    def attend(m):
        mean = jnp.sum(ssq[m], axis=-1, keepdims=True) * (1.0 / D)
        packed = (acc[m] * lax.rsqrt(mean + EPS)).astype(BF)
        q, k, v = packed[:, :PAD], packed[:, PAD:2 * PAD], packed[:, 2 * PAD:]
        scores = lax.dot_general(q, k, (((1,), (1,)), ((), ())), preferred_element_type=F32)
        t = lax.broadcasted_iota(jnp.int32, (TOKENS, TOKENS), 0)
        u = lax.broadcasted_iota(jnp.int32, (TOKENS, TOKENS), 1)
        bits = jnp.where(s % 2 == 0, 64, 63)
        scores = jnp.where(((t ^ u) & bits) == 0, scores * HEAD ** (-0.5), -1e30)
        top = jnp.max(scores, axis=-1, keepdims=True)
        e = jnp.exp(scores - top)
        weights = (e / jnp.sum(e, axis=-1, keepdims=True)).astype(BF)
        att[m, j] = jnp.dot(weights, v, preferred_element_type=F32).astype(BF)
        for k in (4, 2, 6, 3, 5, 1, 7):
            send(att.at[m, j], att.at[m, j], a_ss.at[m], a_rs.at[m], at(s, z, other(j, k)))

    def project(m):
        drain(att.at[m, pl.ds(0, G - 1)], a_rs.at[m])
        together = jnp.concatenate([att[m, g] for g in range(G)], axis=1)
        part[m] = jnp.dot(together, wo[...].reshape(G * PAD, WIDE), preferred_element_type=F32).astype(BF)
        for d in ORDER[::-1][:-1]:
            zz = (z + d) % Z
            send(part.at[m, rows(zz)], rsb.at[m, z], p_ss.at[m], p_rs.at[m], at(s, zz, j))

    def finish(m):
        total = x[m, j, rows(z), :].astype(F32) + part[m, rows(z), :].astype(F32)
        drain(rsb.at[m, pl.ds(0, Z - 1)], p_rs.at[m])
        for d in range(1, Z):
            total += rsb[m, (z + d) % Z].astype(F32)

        @pl.when(s < LAST)
        def _():
            slab[2 + m] = total.astype(BF)
            spread(slab.at[2 + m], m, s + 1, z_ss.at[m], False)

        @pl.when(s == LAST)
        def _():
            for g in range(G):
                fin[m, g] = total[2 * g:2 * g + 2, :]
            columns = pl.ds(pl.multiple_of(c * WIDE, WIDE), WIDE)

            @pl.when(y < LAST)
            def _():
                for g in range(G):
                    send(fin.at[m, g], out_ref.at[m, :, columns], f_ss.at[m], f_rs.at[m, c], at(y, z, g))

            @pl.when(y == LAST)
            def _():
                out_ref[m, :, columns] = fin[m, j]
                for k in range(1, G):
                    to = other(j, k)
                    send(fin.at[m, to], out_ref.at[m, :, columns], f_ss.at[m], f_rs.at[m, c], at(s, z, to))

    take_rows(0)
    take_rows(1)
    take_groups(0)
    attend(0)
    own_wo.wait()
    drain(wo.at[pl.ds(0, G - 1), pl.ds(0, HEAD)], wo_rs)
    project(0)
    take_groups(1)
    attend(1)
    finish(0)
    project(1)
    finish(1)

    drain(wo.at[pl.ds(0, G - 1), pl.ds(0, HEAD)], wo_ss)

    @pl.when(s == 0)
    def _():
        drain(ini_s.at[pl.ds(0, G - 1)], ini_ss)
        for m in range(2):
            drain(x.at[m, 0, pl.ds(0, TOKENS - ROWS)], zi_ss.at[m])

    for m in range(2):
        drain(x.at[m, pl.ds(0, 2)], y_ss.at[m])
        drain(x.at[m, 0], r_ss.at[m])
        drain(x.at[m, pl.ds(0, 4)], d_ss.at[m])
        drain(att.at[m, pl.ds(0, G - 1)], a_ss.at[m])
        drain(rsb.at[m, pl.ds(0, Z - 1)], p_ss.at[m])

        @pl.when(s < LAST)
        def _():
            drain(x.at[m, 0], z_ss.at[m])

        @pl.when(jnp.logical_and(s == LAST, y < LAST))
        def _():
            drain(fin.at[m], f_ss.at[m])

        @pl.when(jnp.logical_and(s == LAST, y == LAST))
        def _():
            drain(fin.at[m, pl.ds(0, G - 1)], f_ss.at[m])

        for k in range(2):
            @pl.when(jnp.logical_not(jnp.logical_and(s == LAST, jnp.logical_and(y == LAST, c == k))))
            def _():
                drain(out_ref.at[m, :, pl.ds(k * WIDE, WIDE)], f_rs.at[m, k])


def per_device(video_tokens, norm_gain, qkv_weight, out_weight):
    vmem = pl.BlockSpec(memory_space=pltpu.VMEM)
    anywhere = pl.BlockSpec(memory_space=pl.ANY)
    dma = pltpu.SemaphoreType.DMA
    return pl.pallas_call(
        kernel,
        out_shape=jax.ShapeDtypeStruct((2, 2, 2 * WIDE), F32),
        in_specs=[vmem, vmem, anywhere, anywhere],
        out_specs=vmem,
        scratch_shapes=[
            pltpu.VMEM((2, G, TOKENS, WIDE), BF),
            pltpu.VMEM((D, 3 * HEAD), BF),
            pltpu.VMEM((G, WIDE, 3 * PAD), BF),
            pltpu.VMEM((G, PAD, WIDE), BF),
            pltpu.VMEM((2, TOKENS, 3 * PAD), F32),
            pltpu.VMEM((2, TOKENS, 128), F32),
            pltpu.VMEM((2, G, TOKENS, PAD), BF),
            pltpu.VMEM((2, TOKENS, WIDE), BF),
            pltpu.VMEM((2, Z, ROWS, WIDE), BF),
            pltpu.VMEM((4, ROWS, WIDE), BF),
            pltpu.VMEM((2, G, 2, WIDE), F32),
            pltpu.VMEM((G, 2, 2, WIDE), F32),
            pltpu.VMEM((G, 2, 2, WIDE), F32),
            dma, dma, dma, dma, dma, dma, dma((2,)), dma((2,)), dma((2, Z)), dma((2,)), dma((2, 2, 2)),
            dma((2,)), dma((2, 2)), dma((2,)), dma((2, 4)), dma((2,)), dma((2,)), dma((2,)), dma((2,)),
            dma((2,)), dma((2, 2)),
        ],
        compiler_params=pltpu.CompilerParams(
            collective_id=0, has_side_effects=True, vmem_limit_bytes=56 * 1024 * 1024
        ),
    )(video_tokens, norm_gain, qkv_weight[0], out_weight[0])


def solution(mesh):
    return jax.shard_map(
        per_device,
        mesh=mesh,
        in_specs=(
            P(None, "mesh", None),
            P("section", None),
            P("section", None, "mesh"),
            P("section", "mesh", None),
        ),
        out_specs=P(None, "mesh", "section"),
        check_vma=False,
    )
```

```python
import jax
import jax.numpy as jnp
from jax import lax
from jax.experimental import pallas as pl
from jax.experimental.pallas import tpu as pltpu
from jax.sharding import PartitionSpec as P

MESH = pl.DeviceIdType.MESH
HEAD = 96
PAD = 128
Z, Y, G = 8, 4, 8
ROWS = 16
WIDE = 768
TOKENS = 128
D = 6144
LAST = 3
EPS = 1e-06
ORDER = (0, 1, 7, 2, 6, 3, 5, 4)
BF = jnp.bfloat16
F32 = jnp.float32


def kernel(
    tok_ref, gain_ref, w_hbm, wo_hbm, out_ref,
    x, wraw, wp, wo, stage, acc, ssq, att, part, rsb, slab, fin, ini_s, ini_r,
    wsem, ini_ss, ini_rs, wo_ss, wo_rs, wo_ls, st_ss, st_rs, zi_ss, z_ss, z_rs, y_ss, y_rs, r_rs,
    d_ss, d_rs, a_ss, a_rs, p_ss, p_rs, f_ss, f_rs,
):
    s = lax.axis_index("section")
    me = lax.axis_index("mesh")
    z, j = me // G, me % G
    y, c = j // 2, j % 2

    def at(sec, zz, jj):
        return (sec, zz * G + jj)

    def send(src, dst, ssem, rsem, dev):
        pltpu.make_async_remote_copy(
            src_ref=src, dst_ref=dst, send_sem=ssem, recv_sem=rsem, device_id=dev, device_id_type=MESH
        ).start()

    def drain(ref, sem):
        pltpu.make_async_copy(ref, ref, sem).wait()

    def rows(zz):
        return pl.ds(pl.multiple_of(zz * ROWS, ROWS), ROWS)

    def other(jj, k):
        return (jj + k) % G

    wcopy = pltpu.make_async_copy(w_hbm, wraw, wsem)
    wcopy.start()
    own_wo = pltpu.make_async_copy(
        wo_hbm.at[:, pl.ds(pl.multiple_of(j * WIDE, WIDE), WIDE)], wo.at[j], wo_ls
    )
    own_wo.start()

    barrier = pltpu.get_barrier_semaphore()

    def greet(dev):
        pl.semaphore_signal(barrier, inc=1, device_id=dev, device_id_type=MESH)

    for k in range(1, G):
        greet(at(s, z, other(j, k)))
    for k in range(1, Z):
        greet(at(s, (z + k) % Z, j))

    @pl.when(s < LAST)
    def _():
        for k in range(Z):
            greet(at(s + 1, k, j))
        for k in range(2):
            greet(at(LAST, z, 2 * s + k))

    @pl.when(s > 0)
    def _():
        for k in range(Z):
            greet(at(s - 1, k, j))

    @pl.when(jnp.logical_and(s == LAST, y < LAST))
    def _():
        for k in range(G):
            greet(at(y, z, k))

    wcopy.wait()

    def prepare(g, carry):
        features = pl.ds(pl.multiple_of(g * WIDE, WIDE), WIDE)
        blank = jnp.zeros((PAD - HEAD, WIDE), F32)
        for q in range(3):
            piece = wraw[q * HEAD:(q + 1) * HEAD, features].astype(F32) * gain_ref[:, features]
            wp[g, :, q * PAD:(q + 1) * PAD] = jnp.concatenate([piece, blank], axis=0).T.astype(BF)
        return carry

    lax.fori_loop(0, G, prepare, 0)

    @pl.when(s == 0)
    def _():
        for g in range(G):
            for m in range(2):
                ini_s[g, m] = tok_ref[m, :, g * WIDE:(g + 1) * WIDE].astype(F32)

    greeted = G - 1 + Z - 1 + jnp.where(s < LAST, Z + 2, 0) + jnp.where(s > 0, Z, 0)
    pl.semaphore_wait(barrier, greeted + jnp.where(jnp.logical_and(s == LAST, y < LAST), G, 0))

    @pl.when(s == 0)
    def _():
        for k in range(1, G):
            to = other(j, k)
            send(ini_s.at[to], ini_r.at[j], ini_ss, ini_rs, at(s, z, to))

    def share_wo(dy, cc, to=None, dst=None, rsem=None):
        goal = (y + dy) % Y * 2 + cc
        columns = pl.ds(pl.multiple_of(goal * WIDE, WIDE), WIDE)
        if to is None:
            to, dst, rsem = goal, wo.at[j], wo_rs
        send(wo_hbm.at[:, columns], dst, wo_ss, rsem, at(s, z, to))

    share_wo(2, 1 - c, other(j, 6), stage, st_rs)
    share_wo(0, 1 - c)
    share_wo(1, c)
    share_wo(3, c)

    def share_wo_rest():
        share_wo(2, c)
        share_wo(1, 1 - c)
        share_wo(3, 1 - c)
        drain(stage, st_rs)
        send(stage, wo.at[other(j, 2)], st_ss, wo_rs, at(s, z, other(j, 6) + 1 - 2 * c))

    @pl.when(s > 0)
    def _():
        share_wo_rest()

    def spread(src, m, sec, ssem, skip_own):
        for d in ORDER:
            if d == 0 and skip_own:
                continue
            send(src, x.at[m, j, rows(z)], ssem, z_rs.at[m, z], at(sec, (z + d) % Z, j))

    @pl.when(s == 0)
    def _():
        ini_r[j] = ini_s[j]
        drain(ini_r.at[pl.ds(0, G - 1)], ini_rs)
        for m in range(2):
            whole = jnp.concatenate([ini_r[g, m] for g in range(G)], axis=0).astype(BF)
            slab[m] = whole
            x[m, j, rows(z), :] = whole
            spread(slab.at[m], m, s, zi_ss.at[m], True)

    def take_rows(m):
        for i, d in enumerate(ORDER):
            zz = (z + d) % Z
            chunk = x.at[m, j, rows(zz)]
            if d == 0:
                @pl.when(s > 0)
                def _():
                    drain(chunk, z_rs.at[m, zz])
            else:
                drain(chunk, z_rs.at[m, zz])
            half = 0 if i < 4 else 1
            send(chunk, chunk, y_ss.at[m], y_rs.at[m, 0, half], at(s, z, other(j, 2)))
            send(chunk, chunk, y_ss.at[m], y_rs.at[m, 1, half], at(s, z, other(j, 6)))
            send(chunk, chunk, y_ss.at[m], r_rs.at[m, half], at(s, z, other(j, 4)))
        share(m, 0, j)

    def sibling(jj):
        return jj + 1 - 2 * c

    def share(m, slot, jj):
        send(x.at[m, jj], x.at[m, jj], d_ss.at[m], d_rs.at[m, slot], at(s, z, sibling(j)))

    def multiply(m, jj, first=False):
        xs = x[m, jj]
        wide = xs.astype(F32)
        squares = wide * wide
        total = squares[:, :128]
        for i in range(1, WIDE // 128):
            total += squares[:, i * 128:(i + 1) * 128]
        product = jnp.dot(xs, wp[jj], preferred_element_type=F32)
        if first:
            acc[m] = product
            ssq[m] = total
        else:
            acc[m] += product
            ssq[m] += total

    def take_groups(m):
        before, after, across = other(j, 6), other(j, 2), other(j, 4)
        half_rows = pl.ds(0, TOKENS // 2)
        multiply(m, j, True)
        for half in range(2):
            drain(x.at[m, after, half_rows], y_rs.at[m, 1, half])
        share(m, 1, after)
        for half in range(2):
            drain(x.at[m, before, half_rows], y_rs.at[m, 0, half])
        share(m, 2, before)
        for half in range(2):
            drain(x.at[m, across, half_rows], r_rs.at[m, half])
        share(m, 3, across)
        multiply(m, after)
        multiply(m, before)
        multiply(m, across)
        for slot, jj in ((0, j), (1, after), (2, before), (3, across)):
            drain(x.at[m, jj], d_rs.at[m, slot])
            multiply(m, sibling(jj))

    def attend(m):
        mean = jnp.sum(ssq[m], axis=-1, keepdims=True) * (1.0 / D)
        packed = (acc[m] * lax.rsqrt(mean + EPS)).astype(BF)
        q, k, v = packed[:, :PAD], packed[:, PAD:2 * PAD], packed[:, 2 * PAD:]
        scores = lax.dot_general(q, k, (((1,), (1,)), ((), ())), preferred_element_type=F32)
        t = lax.broadcasted_iota(jnp.int32, (TOKENS, TOKENS), 0)
        u = lax.broadcasted_iota(jnp.int32, (TOKENS, TOKENS), 1)
        bits = jnp.where(s % 2 == 0, 64, 63)
        scores = jnp.where(((t ^ u) & bits) == 0, scores * HEAD ** (-0.5), -1e30)
        top = jnp.max(scores, axis=-1, keepdims=True)
        e = jnp.exp(scores - top)
        weights = (e / jnp.sum(e, axis=-1, keepdims=True)).astype(BF)
        across = lax.dot_general(v, weights, (((0,), (1,)), ((), ())), preferred_element_type=F32)
        att[m, j] = across[:HEAD].astype(BF)
        for k in (4, 2, 6, 3, 5, 1, 7):
            send(att.at[m, j], att.at[m, j], a_ss.at[m], a_rs.at[m], at(s, z, other(j, k)))

    def project(m):
        drain(att.at[m, pl.ds(0, G - 1)], a_rs.at[m])
        together = att[m].reshape(G * HEAD, TOKENS)
        product = lax.dot_general(together, wo[...].reshape(G * HEAD, WIDE), (((0,), (0,)), ((), ())), preferred_element_type=F32)
        part[m] = product.astype(BF)
        for d in ORDER[::-1][:-1]:
            zz = (z + d) % Z
            send(part.at[m, rows(zz)], rsb.at[m, z], p_ss.at[m], p_rs.at[m], at(s, zz, j))

    def finish(m):
        total = x[m, j, rows(z), :].astype(F32) + part[m, rows(z), :].astype(F32)
        drain(rsb.at[m, pl.ds(0, Z - 1)], p_rs.at[m])
        for d in range(1, Z):
            total += rsb[m, (z + d) % Z].astype(F32)

        @pl.when(s < LAST)
        def _():
            slab[2 + m] = total.astype(BF)
            spread(slab.at[2 + m], m, s + 1, z_ss.at[m], False)

        @pl.when(s == LAST)
        def _():
            for g in range(G):
                fin[m, g] = total[2 * g:2 * g + 2, :]
            columns = pl.ds(pl.multiple_of(c * WIDE, WIDE), WIDE)

            @pl.when(y < LAST)
            def _():
                for g in range(G):
                    send(fin.at[m, g], out_ref.at[m, :, columns], f_ss.at[m], f_rs.at[m, c], at(y, z, g))

            @pl.when(y == LAST)
            def _():
                out_ref[m, :, columns] = fin[m, j]
                for k in range(1, G):
                    to = other(j, k)
                    send(fin.at[m, to], out_ref.at[m, :, columns], f_ss.at[m], f_rs.at[m, c], at(s, z, to))

    take_rows(0)

    @pl.when(s == 0)
    def _():
        share_wo_rest()

    take_groups(0)
    attend(0)
    own_wo.wait()
    drain(wo.at[pl.ds(0, G - 1)], wo_rs)
    project(0)
    take_rows(1)
    finish(0)
    take_groups(1)
    attend(1)
    project(1)
    finish(1)

    drain(wo.at[pl.ds(0, G - 1)], wo_ss)
    drain(stage, st_ss)

    @pl.when(s == 0)
    def _():
        drain(ini_s.at[pl.ds(0, G - 1)], ini_ss)
        for m in range(2):
            drain(x.at[m, 0, pl.ds(0, TOKENS - ROWS)], zi_ss.at[m])

    for m in range(2):
        drain(x.at[m, pl.ds(0, 3)], y_ss.at[m])
        drain(x.at[m, pl.ds(0, 4)], d_ss.at[m])
        drain(att.at[m, pl.ds(0, G - 1)], a_ss.at[m])
        drain(rsb.at[m, pl.ds(0, Z - 1)], p_ss.at[m])

        @pl.when(s < LAST)
        def _():
            drain(x.at[m, 0], z_ss.at[m])

        @pl.when(jnp.logical_and(s == LAST, y < LAST))
        def _():
            drain(fin.at[m], f_ss.at[m])

        @pl.when(jnp.logical_and(s == LAST, y == LAST))
        def _():
            drain(fin.at[m, pl.ds(0, G - 1)], f_ss.at[m])

        for k in range(2):
            @pl.when(jnp.logical_not(jnp.logical_and(s == LAST, jnp.logical_and(y == LAST, c == k))))
            def _():
                drain(out_ref.at[m, :, pl.ds(k * WIDE, WIDE)], f_rs.at[m, k])


def per_device(video_tokens, norm_gain, qkv_weight, out_weight):
    vmem = pl.BlockSpec(memory_space=pltpu.VMEM)
    anywhere = pl.BlockSpec(memory_space=pl.ANY)
    dma = pltpu.SemaphoreType.DMA
    return pl.pallas_call(
        kernel,
        out_shape=jax.ShapeDtypeStruct((2, 2, 2 * WIDE), F32),
        in_specs=[vmem, vmem, anywhere, anywhere],
        out_specs=vmem,
        scratch_shapes=[
            pltpu.VMEM((2, G, TOKENS, WIDE), BF),
            pltpu.VMEM((3 * HEAD, D), BF),
            pltpu.VMEM((G, WIDE, 3 * PAD), BF),
            pltpu.VMEM((G, HEAD, WIDE), BF),
            pltpu.VMEM((HEAD, WIDE), BF),
            pltpu.VMEM((2, TOKENS, 3 * PAD), F32),
            pltpu.VMEM((2, TOKENS, 128), F32),
            pltpu.VMEM((2, G, HEAD, TOKENS), BF),
            pltpu.VMEM((2, TOKENS, WIDE), BF),
            pltpu.VMEM((2, Z, ROWS, WIDE), BF),
            pltpu.VMEM((4, ROWS, WIDE), BF),
            pltpu.VMEM((2, G, 2, WIDE), F32),
            pltpu.VMEM((G, 2, 2, WIDE), F32),
            pltpu.VMEM((G, 2, 2, WIDE), F32),
            dma, dma, dma, dma, dma, dma, dma, dma, dma((2,)), dma((2,)), dma((2, Z)), dma((2,)), dma((2, 2, 2)),
            dma((2, 2)), dma((2,)), dma((2, 4)), dma((2,)), dma((2,)), dma((2,)), dma((2,)),
            dma((2,)), dma((2, 2)),
        ],
        compiler_params=pltpu.CompilerParams(
            collective_id=0, has_side_effects=True, vmem_limit_bytes=56 * 1024 * 1024
        ),
    )(video_tokens, norm_gain, qkv_weight[0].T, out_weight[0])


def solution(mesh):
    return jax.shard_map(
        per_device,
        mesh=mesh,
        in_specs=(
            P(None, "mesh", None),
            P("section", None),
            P("section", None, "mesh"),
            P("section", "mesh", None),
        ),
        out_specs=P(None, "mesh", "section"),
        check_vma=False,
    )
```

```python
import jax
import jax.numpy as jnp
from jax import lax
from jax.experimental import pallas as pl
from jax.experimental.pallas import tpu as pltpu
from jax.sharding import PartitionSpec as P

MESH = pl.DeviceIdType.MESH
HEAD = 96
PAD = 128
Z, Y, G = 8, 4, 8
ROWS = 16
WIDE = 768
TOKENS = 128
D = 6144
LAST = 3
EPS = 1e-06
ORDER = (0, 1, 7, 2, 6, 3, 5, 4)
BF = jnp.bfloat16
F32 = jnp.float32


def kernel(
    tok_ref, gain_ref, w_hbm, wo_hbm, out_ref,
    x, wraw, wp, wo, lent, moved, acc, ssq, att, part, rsb, slab, fin, ini_s, ini_r,
    wsem, ini_ss, ini_rs, wo_ss, wo_rs, wo_ls, near, far, ahead, l_rs, m_ss, m_rs, zi_ss, z_ss, z_rs, y_ss, y_rs, r_rs,
    d_ss, d_rs, a_ss, a_rs, p_ss, p_rs, f_ss, f_rs,
):
    s = lax.axis_index("section")
    me = lax.axis_index("mesh")
    z, j = me // G, me % G
    y, c = j // 2, j % 2

    def at(sec, zz, jj):
        return (sec, zz * G + jj)

    def send(src, dst, ssem, rsem, dev):
        pltpu.make_async_remote_copy(
            src_ref=src, dst_ref=dst, send_sem=ssem, recv_sem=rsem, device_id=dev, device_id_type=MESH
        ).start()

    def drain(ref, sem):
        pltpu.make_async_copy(ref, ref, sem).wait()

    def rows(zz):
        return pl.ds(pl.multiple_of(zz * ROWS, ROWS), ROWS)

    def other(jj, k):
        return (jj + k) % G

    wcopy = pltpu.make_async_copy(w_hbm, wraw, wsem)
    wcopy.start()
    own_wo = pltpu.make_async_copy(
        wo_hbm.at[:, pl.ds(pl.multiple_of(j * WIDE, WIDE), WIDE)], wo.at[j], wo_ls
    )
    own_wo.start()

    barrier = pltpu.get_barrier_semaphore()

    def signal(sem, dev):
        pl.semaphore_signal(sem, inc=1, device_id=dev, device_id_type=MESH)

    for k in range(1, G):
        signal(barrier, at(s, z, other(j, k)))
    for k in (1, Z - 1):
        signal(barrier, at(s, (z + k) % Z, j))
    for k in (1, LAST):
        signal(barrier, at((s + k) % (LAST + 1), z, j))

    wcopy.wait()

    def prepare(g, carry):
        features = pl.ds(pl.multiple_of(g * WIDE, WIDE), WIDE)
        blank = jnp.zeros((PAD - HEAD, WIDE), F32)
        for q in range(3):
            piece = wraw[q * HEAD:(q + 1) * HEAD, features].astype(F32) * gain_ref[:, features]
            wp[g, :, q * PAD:(q + 1) * PAD] = jnp.concatenate([piece, blank], axis=0).T.astype(BF)
        return carry

    lax.fori_loop(0, G, prepare, 0)

    @pl.when(s == 0)
    def _():
        for g in range(G):
            for m in range(2):
                ini_s[g, m] = tok_ref[m, :, g * WIDE:(g + 1) * WIDE].astype(F32)

    pl.semaphore_wait(barrier, G - 1 + 4)

    @pl.when(s == 0)
    def _():
        for k in range(1, G):
            to = other(j, k)
            send(ini_s.at[to], ini_r.at[j], ini_ss, ini_rs, at(s, z, to))

    for k in (1, Z - 1):
        signal(near, at(s, (z + k) % Z, j))

    def columns(goal):
        return pl.ds(pl.multiple_of(goal * WIDE, WIDE), WIDE)

    def share_wo(dy, cc):
        goal = (y + dy) % Y * 2 + cc
        send(wo_hbm.at[:, columns(goal)], wo.at[j], wo_ss, wo_rs, at(s, z, goal))

    def lend_wo(dy, cc, sec, i):
        goal = (y + dy) % Y * 2 + cc
        send(wo_hbm.at[:, columns(goal)], lent.at[i], wo_ss, l_rs.at[i], at(sec, z, j))

    share_wo(0, 1 - c)

    @pl.when(s == 0)
    def _():
        share_wo(1, c)
        share_wo(3, c)
        lend_wo(2, c, LAST, 0)
        lend_wo(1, 1 - c, 1, 0)
        lend_wo(2, 1 - c, LAST, 1)
        lend_wo(3, 1 - c, 1, 1)

    pl.semaphore_wait(near, 2)
    for k in (2, Z - 2):
        signal(far, at(s, (z + k) % Z, j))
    pl.semaphore_wait(far, 2)

    @pl.when(s > 0)
    def _():
        signal(ahead, at(s - 1, z, j))

        @pl.when(s != 2)
        def _():
            for i in range(2):
                dy = jnp.where(s == 1, 1 + 2 * i, 2)
                cc = jnp.where(s == 1, 1 - c, c + i * (1 - 2 * c))
                drain(lent.at[i], l_rs.at[i])
                send(lent.at[i], moved.at[i], m_ss, m_rs.at[i], at(s, z, (y + dy) % Y * 2 + cc))
            for i in range(2):
                dy = jnp.where(s == 1, 1 + 2 * i, 2)
                cc = jnp.where(s == 1, 1 - c, c + i * (1 - 2 * c))
                drain(moved.at[i], m_rs.at[i])
                send(moved.at[i], wo.at[(y + Y - dy) % Y * 2 + cc], m_ss, wo_rs, at(0, z, j))

        for dy, cc in ((2, c), (1, c), (3, c), (2, 1 - c), (1, 1 - c), (3, 1 - c)):
            share_wo(dy, cc)

    def spread(src, m, sec, ssem, skip_own):
        for d in ORDER:
            if d == 0 and skip_own:
                continue
            send(src, x.at[m, j, rows(z)], ssem, z_rs.at[m, z], at(sec, (z + d) % Z, j))

    @pl.when(s == 0)
    def _():
        ini_r[j] = ini_s[j]
        drain(ini_r.at[pl.ds(0, G - 1)], ini_rs)
        for m in range(2):
            whole = jnp.concatenate([ini_r[g, m] for g in range(G)], axis=0).astype(BF)
            slab[m] = whole
            x[m, j, rows(z), :] = whole
            spread(slab.at[m], m, s, zi_ss.at[m], True)

    def take_rows(m):
        for i, d in enumerate(ORDER):
            zz = (z + d) % Z
            chunk = x.at[m, j, rows(zz)]
            if d == 0:
                @pl.when(s > 0)
                def _():
                    drain(chunk, z_rs.at[m, zz])
            else:
                drain(chunk, z_rs.at[m, zz])
            half = 0 if i < 4 else 1
            send(chunk, chunk, y_ss.at[m], y_rs.at[m, 0, half], at(s, z, other(j, 2)))
            send(chunk, chunk, y_ss.at[m], y_rs.at[m, 1, half], at(s, z, other(j, 6)))
            send(chunk, chunk, y_ss.at[m], r_rs.at[m, half], at(s, z, other(j, 4)))
        share(m, 0, j)

    def sibling(jj):
        return jj + 1 - 2 * c

    def share(m, slot, jj):
        send(x.at[m, jj], x.at[m, jj], d_ss.at[m], d_rs.at[m, slot], at(s, z, sibling(j)))

    def multiply(m, jj, first=False):
        xs = x[m, jj]
        wide = xs.astype(F32)
        squares = wide * wide
        total = squares[:, :128]
        for i in range(1, WIDE // 128):
            total += squares[:, i * 128:(i + 1) * 128]
        product = jnp.dot(xs, wp[jj], preferred_element_type=F32)
        if first:
            acc[m] = product
            ssq[m] = total
        else:
            acc[m] += product
            ssq[m] += total

    def take_groups(m):
        before, after, across = other(j, 6), other(j, 2), other(j, 4)
        half_rows = pl.ds(0, TOKENS // 2)
        multiply(m, j, True)
        for half in range(2):
            drain(x.at[m, after, half_rows], y_rs.at[m, 1, half])
        share(m, 1, after)
        for half in range(2):
            drain(x.at[m, before, half_rows], y_rs.at[m, 0, half])
        share(m, 2, before)
        for half in range(2):
            drain(x.at[m, across, half_rows], r_rs.at[m, half])
        share(m, 3, across)
        multiply(m, after)
        multiply(m, before)
        multiply(m, across)
        for slot, jj in ((0, j), (1, after), (2, before), (3, across)):
            drain(x.at[m, jj], d_rs.at[m, slot])
            multiply(m, sibling(jj))

    def attend(m):
        mean = jnp.sum(ssq[m], axis=-1, keepdims=True) * (1.0 / D)
        packed = (acc[m] * lax.rsqrt(mean + EPS)).astype(BF)
        q, k, v = packed[:, :PAD], packed[:, PAD:2 * PAD], packed[:, 2 * PAD:]
        scores = lax.dot_general(q, k, (((1,), (1,)), ((), ())), preferred_element_type=F32)
        t = lax.broadcasted_iota(jnp.int32, (TOKENS, TOKENS), 0)
        u = lax.broadcasted_iota(jnp.int32, (TOKENS, TOKENS), 1)
        bits = jnp.where(s % 2 == 0, 64, 63)
        scores = jnp.where(((t ^ u) & bits) == 0, scores * HEAD ** (-0.5), -1e30)
        top = jnp.max(scores, axis=-1, keepdims=True)
        e = jnp.exp(scores - top)
        weights = (e / jnp.sum(e, axis=-1, keepdims=True)).astype(BF)
        across = lax.dot_general(v, weights, (((0,), (1,)), ((), ())), preferred_element_type=F32)
        att[m, j] = across[:HEAD].astype(BF)
        for k in (2, 6, 3, 5, 4, 1, 7):
            send(att.at[m, j], att.at[m, j], a_ss.at[m], a_rs.at[m], at(s, z, other(j, k)))

    def project(m):
        drain(att.at[m, pl.ds(0, G - 1)], a_rs.at[m])
        together = att[m].reshape(G * HEAD, TOKENS)
        product = lax.dot_general(together, wo[...].reshape(G * HEAD, WIDE), (((0,), (0,)), ((), ())), preferred_element_type=F32)
        part[m] = product.astype(BF)
        for d in ORDER[::-1][:-1]:
            zz = (z + d) % Z
            send(part.at[m, rows(zz)], rsb.at[m, z], p_ss.at[m], p_rs.at[m], at(s, zz, j))

    def finish(m):
        total = x[m, j, rows(z), :].astype(F32) + part[m, rows(z), :].astype(F32)
        drain(rsb.at[m, pl.ds(0, Z - 1)], p_rs.at[m])
        for d in range(1, Z):
            total += rsb[m, (z + d) % Z].astype(F32)

        @pl.when(s < LAST)
        def _():
            if m == 0:
                pl.semaphore_wait(ahead, 1)
            slab[2 + m] = total.astype(BF)
            spread(slab.at[2 + m], m, s + 1, z_ss.at[m], False)

        @pl.when(s == LAST)
        def _():
            for g in range(G):
                fin[m, g] = total[2 * g:2 * g + 2, :]
            columns = pl.ds(pl.multiple_of(c * WIDE, WIDE), WIDE)

            @pl.when(y < LAST)
            def _():
                for g in range(G):
                    send(fin.at[m, g], out_ref.at[m, :, columns], f_ss.at[m], f_rs.at[m, c], at(y, z, g))

            @pl.when(y == LAST)
            def _():
                out_ref[m, :, columns] = fin[m, j]
                for k in range(1, G):
                    to = other(j, k)
                    send(fin.at[m, to], out_ref.at[m, :, columns], f_ss.at[m], f_rs.at[m, c], at(s, z, to))

    take_rows(0)

    take_groups(0)
    attend(0)
    own_wo.wait()
    drain(wo.at[pl.ds(0, G - 1)], wo_rs)
    project(0)
    take_rows(1)
    finish(0)
    take_groups(1)
    attend(1)
    project(1)
    finish(1)

    drain(wo.at[pl.ds(0, G - 1)], wo_ss)

    @pl.when(jnp.logical_or(s == 1, s == LAST))
    def _():
        drain(wo.at[pl.ds(0, 4)], m_ss)


    @pl.when(s == 0)
    def _():
        drain(ini_s.at[pl.ds(0, G - 1)], ini_ss)
        for m in range(2):
            drain(x.at[m, 0, pl.ds(0, TOKENS - ROWS)], zi_ss.at[m])

    for m in range(2):
        drain(x.at[m, pl.ds(0, 3)], y_ss.at[m])
        drain(x.at[m, pl.ds(0, 4)], d_ss.at[m])
        drain(att.at[m, pl.ds(0, G - 1)], a_ss.at[m])
        drain(rsb.at[m, pl.ds(0, Z - 1)], p_ss.at[m])

        @pl.when(s < LAST)
        def _():
            drain(x.at[m, 0], z_ss.at[m])

        @pl.when(jnp.logical_and(s == LAST, y < LAST))
        def _():
            drain(fin.at[m], f_ss.at[m])

        @pl.when(jnp.logical_and(s == LAST, y == LAST))
        def _():
            drain(fin.at[m, pl.ds(0, G - 1)], f_ss.at[m])

        for k in range(2):
            @pl.when(jnp.logical_not(jnp.logical_and(s == LAST, jnp.logical_and(y == LAST, c == k))))
            def _():
                drain(out_ref.at[m, :, pl.ds(k * WIDE, WIDE)], f_rs.at[m, k])


def per_device(video_tokens, norm_gain, qkv_weight, out_weight):
    vmem = pl.BlockSpec(memory_space=pltpu.VMEM)
    anywhere = pl.BlockSpec(memory_space=pl.ANY)
    dma, regular = pltpu.SemaphoreType.DMA, pltpu.SemaphoreType.REGULAR
    return pl.pallas_call(
        kernel,
        out_shape=jax.ShapeDtypeStruct((2, 2, 2 * WIDE), F32),
        in_specs=[vmem, vmem, anywhere, anywhere],
        out_specs=vmem,
        scratch_shapes=[
            pltpu.VMEM((2, G, TOKENS, WIDE), BF),
            pltpu.VMEM((3 * HEAD, D), BF),
            pltpu.VMEM((G, WIDE, 3 * PAD), BF),
            pltpu.VMEM((G, HEAD, WIDE), BF),
            pltpu.VMEM((2, HEAD, WIDE), BF),
            pltpu.VMEM((2, HEAD, WIDE), BF),
            pltpu.VMEM((2, TOKENS, 3 * PAD), F32),
            pltpu.VMEM((2, TOKENS, 128), F32),
            pltpu.VMEM((2, G, HEAD, TOKENS), BF),
            pltpu.VMEM((2, TOKENS, WIDE), BF),
            pltpu.VMEM((2, Z, ROWS, WIDE), BF),
            pltpu.VMEM((4, ROWS, WIDE), BF),
            pltpu.VMEM((2, G, 2, WIDE), F32),
            pltpu.VMEM((G, 2, 2, WIDE), F32),
            pltpu.VMEM((G, 2, 2, WIDE), F32),
            dma, dma, dma, dma, dma, dma, regular, regular, regular, dma((2,)), dma, dma((2,)),
            dma((2,)), dma((2,)), dma((2, Z)), dma((2,)), dma((2, 2, 2)),
            dma((2, 2)), dma((2,)), dma((2, 4)), dma((2,)), dma((2,)), dma((2,)), dma((2,)),
            dma((2,)), dma((2, 2)),
        ],
        compiler_params=pltpu.CompilerParams(
            collective_id=0, has_side_effects=True, vmem_limit_bytes=56 * 1024 * 1024
        ),
    )(video_tokens, norm_gain, qkv_weight[0].T, out_weight[0])


def solution(mesh):
    return jax.shard_map(
        per_device,
        mesh=mesh,
        in_specs=(
            P(None, "mesh", None),
            P("section", None),
            P("section", None, "mesh"),
            P("section", "mesh", None),
        ),
        out_specs=P(None, "mesh", "section"),
        check_vma=False,
    )
```

```python
import jax
import jax.numpy as jnp
from jax import lax
from jax.experimental import pallas as pl
from jax.experimental.pallas import tpu as pltpu
from jax.sharding import PartitionSpec as P

MESH = pl.DeviceIdType.MESH
HEAD = 96
PAD = 128
Z, Y, G = 8, 4, 8
ROWS = 16
WIDE = 768
TOKENS = 128
D = 6144
LAST = 3
EPS = 1e-06
ORDER = (0, 1, 7, 2, 6, 3, 5, 4)
BF = jnp.bfloat16
F32 = jnp.float32


def kernel(
    tok_hbm, gain_hbm, w_hbm, wo_hbm, out_ref,
    tok_ref, gain_ref, x, wraw, wp, wo, lent, moved, acc, ssq, att, part, rsb, slab, fin, ini_s, ini_r,
    tsem, gsem, wsem, ini_ss, ini_rs, wo_ss, wo_rs, wo_ls, near, far, ahead, l_rs, m_ss, m_rs, zi_ss, z_ss, z_rs, y_ss, y_rs, r_rs,
    d_ss, d_rs, a_ss, a_rs, p_ss, p_rs, f_ss, f_rs,
):
    s = lax.axis_index("section")
    me = lax.axis_index("mesh")
    z, j = me // G, me % G
    y, c = j // 2, j % 2

    def at(sec, zz, jj):
        return (sec, zz * G + jj)

    def send(src, dst, ssem, rsem, dev):
        pltpu.make_async_remote_copy(
            src_ref=src, dst_ref=dst, send_sem=ssem, recv_sem=rsem, device_id=dev, device_id_type=MESH
        ).start()

    def drain(ref, sem):
        pltpu.make_async_copy(ref, ref, sem).wait()

    def rows(zz):
        return pl.ds(pl.multiple_of(zz * ROWS, ROWS), ROWS)

    def other(jj, k):
        return (jj + k) % G

    wcopy = pltpu.make_async_copy(w_hbm, wraw, wsem)
    wcopy.start()
    gcopy = pltpu.make_async_copy(gain_hbm, gain_ref, gsem)
    gcopy.start()
    tcopy = pltpu.make_async_copy(tok_hbm, tok_ref, tsem)
    tcopy.start()
    own_wo = pltpu.make_async_copy(
        wo_hbm.at[:, pl.ds(pl.multiple_of(j * WIDE, WIDE), WIDE)], wo.at[j], wo_ls
    )
    own_wo.start()

    barrier = pltpu.get_barrier_semaphore()

    def signal(sem, dev):
        pl.semaphore_signal(sem, inc=1, device_id=dev, device_id_type=MESH)

    for k in range(1, G):
        signal(barrier, at(s, z, other(j, k)))
    for k in (1, Z - 1):
        signal(barrier, at(s, (z + k) % Z, j))
    for k in (1, LAST):
        signal(barrier, at((s + k) % (LAST + 1), z, j))

    tcopy.wait()

    @pl.when(s == 0)
    def _():
        for g in range(G):
            for m in range(2):
                ini_s[g, m] = tok_ref[m, :, g * WIDE:(g + 1) * WIDE].astype(F32)

    pl.semaphore_wait(barrier, G - 1 + 4)

    @pl.when(s == 0)
    def _():
        for k in range(1, G):
            to = other(j, k)
            send(ini_s.at[to], ini_r.at[j], ini_ss, ini_rs, at(s, z, to))

    for k in (1, Z - 1):
        signal(near, at(s, (z + k) % Z, j))

    def columns(goal):
        return pl.ds(pl.multiple_of(goal * WIDE, WIDE), WIDE)

    def share_wo(dy, cc):
        goal = (y + dy) % Y * 2 + cc
        send(wo_hbm.at[:, columns(goal)], wo.at[j], wo_ss, wo_rs, at(s, z, goal))

    def lend_wo(dy, cc, sec, i):
        goal = (y + dy) % Y * 2 + cc
        send(wo_hbm.at[:, columns(goal)], lent.at[i], wo_ss, l_rs.at[i], at(sec, z, j))

    share_wo(0, 1 - c)

    @pl.when(s == 0)
    def _():
        share_wo(1, c)
        share_wo(3, c)
        lend_wo(2, c, LAST, 0)
        lend_wo(1, 1 - c, 1, 0)
        lend_wo(2, 1 - c, LAST, 1)
        lend_wo(3, 1 - c, 1, 1)

    gcopy.wait()
    wcopy.wait()

    def prepare(g, carry):
        features = pl.ds(pl.multiple_of(g * WIDE, WIDE), WIDE)
        blank = jnp.zeros((PAD - HEAD, WIDE), F32)
        for q in range(3):
            piece = wraw[q * HEAD:(q + 1) * HEAD, features].astype(F32) * gain_ref[:, features]
            wp[g, :, q * PAD:(q + 1) * PAD] = jnp.concatenate([piece, blank], axis=0).T.astype(BF)
        return carry

    lax.fori_loop(0, G, prepare, 0)

    pl.semaphore_wait(near, 2)
    for k in (2, Z - 2):
        signal(far, at(s, (z + k) % Z, j))
    pl.semaphore_wait(far, 2)

    @pl.when(s > 0)
    def _():
        signal(ahead, at(s - 1, z, j))

        @pl.when(s != 2)
        def _():
            for i in range(2):
                dy = jnp.where(s == 1, 1 + 2 * i, 2)
                cc = jnp.where(s == 1, 1 - c, c + i * (1 - 2 * c))
                drain(lent.at[i], l_rs.at[i])
                send(lent.at[i], moved.at[i], m_ss, m_rs.at[i], at(s, z, (y + dy) % Y * 2 + cc))
            for i in range(2):
                dy = jnp.where(s == 1, 1 + 2 * i, 2)
                cc = jnp.where(s == 1, 1 - c, c + i * (1 - 2 * c))
                drain(moved.at[i], m_rs.at[i])
                send(moved.at[i], wo.at[(y + Y - dy) % Y * 2 + cc], m_ss, wo_rs, at(0, z, j))

        for dy, cc in ((2, c), (1, c), (3, c), (2, 1 - c), (1, 1 - c), (3, 1 - c)):
            share_wo(dy, cc)

    def spread(src, m, sec, ssem, skip_own):
        for d in ORDER:
            if d == 0 and skip_own:
                continue
            send(src, x.at[m, j, rows(z)], ssem, z_rs.at[m, z], at(sec, (z + d) % Z, j))

    @pl.when(s == 0)
    def _():
        ini_r[j] = ini_s[j]
        drain(ini_r.at[pl.ds(0, G - 1)], ini_rs)
        for m in range(2):
            whole = jnp.concatenate([ini_r[g, m] for g in range(G)], axis=0).astype(BF)
            slab[m] = whole
            x[m, j, rows(z), :] = whole
            spread(slab.at[m], m, s, zi_ss.at[m], True)

    def take_rows(m):
        for i, d in enumerate(ORDER):
            zz = (z + d) % Z
            chunk = x.at[m, j, rows(zz)]
            if d == 0:
                @pl.when(s > 0)
                def _():
                    drain(chunk, z_rs.at[m, zz])
            else:
                drain(chunk, z_rs.at[m, zz])
            half = 0 if i < 4 else 1
            send(chunk, chunk, y_ss.at[m], r_rs.at[m, half], at(s, z, other(j, 4)))
            send(chunk, chunk, y_ss.at[m], y_rs.at[m, 0, half], at(s, z, other(j, 2)))
            send(chunk, chunk, y_ss.at[m], y_rs.at[m, 1, half], at(s, z, other(j, 6)))
        share(m, 0, j)

    def sibling(jj):
        return jj + 1 - 2 * c

    def share(m, slot, jj):
        send(x.at[m, jj], x.at[m, jj], d_ss.at[m], d_rs.at[m, slot], at(s, z, sibling(j)))

    def multiply(m, jj, first=False):
        xs = x[m, jj]
        wide = xs.astype(F32)
        squares = wide * wide
        total = squares[:, :128]
        for i in range(1, WIDE // 128):
            total += squares[:, i * 128:(i + 1) * 128]
        product = jnp.dot(xs, wp[jj], preferred_element_type=F32)
        if first:
            acc[m] = product
            ssq[m] = total
        else:
            acc[m] += product
            ssq[m] += total

    def take_groups(m):
        before, after, across = other(j, 6), other(j, 2), other(j, 4)
        half_rows = pl.ds(0, TOKENS // 2)
        multiply(m, j, True)
        for half in range(2):
            drain(x.at[m, after, half_rows], y_rs.at[m, 1, half])
        share(m, 1, after)
        multiply(m, after)
        for half in range(2):
            drain(x.at[m, before, half_rows], y_rs.at[m, 0, half])
        share(m, 2, before)
        drain(x.at[m, j], d_rs.at[m, 0])
        multiply(m, sibling(j))
        multiply(m, before)
        for half in range(2):
            drain(x.at[m, across, half_rows], r_rs.at[m, half])
        share(m, 3, across)
        drain(x.at[m, after], d_rs.at[m, 1])
        multiply(m, sibling(after))
        multiply(m, across)
        drain(x.at[m, before], d_rs.at[m, 2])
        multiply(m, sibling(before))
        drain(x.at[m, across], d_rs.at[m, 3])
        multiply(m, sibling(across))

    def attend(m):
        mean = jnp.sum(ssq[m], axis=-1, keepdims=True) * (1.0 / D)
        packed = (acc[m] * lax.rsqrt(mean + EPS)).astype(BF)
        q, k, v = packed[:, :PAD], packed[:, PAD:2 * PAD], packed[:, 2 * PAD:]
        scores = lax.dot_general(q, k, (((1,), (1,)), ((), ())), preferred_element_type=F32)
        t = lax.broadcasted_iota(jnp.int32, (TOKENS, TOKENS), 0)
        u = lax.broadcasted_iota(jnp.int32, (TOKENS, TOKENS), 1)
        bits = jnp.where(s % 2 == 0, 64, 63)
        scores = jnp.where(((t ^ u) & bits) == 0, scores * HEAD ** (-0.5), -1e30)
        top = jnp.max(scores, axis=-1, keepdims=True)
        e = jnp.exp(scores - top)
        weights = (e / jnp.sum(e, axis=-1, keepdims=True)).astype(BF)
        across = lax.dot_general(v, weights, (((0,), (1,)), ((), ())), preferred_element_type=F32)
        att[m, j] = across[:HEAD].astype(BF)
        for k in (2, 6, 3, 5, 4, 1, 7):
            send(att.at[m, j], att.at[m, j], a_ss.at[m], a_rs.at[m], at(s, z, other(j, k)))

    def project(m):
        drain(att.at[m, pl.ds(0, G - 1)], a_rs.at[m])
        together = att[m].reshape(G * HEAD, TOKENS)
        product = lax.dot_general(together, wo[...].reshape(G * HEAD, WIDE), (((0,), (0,)), ((), ())), preferred_element_type=F32)
        part[m] = product.astype(BF)
        for d in ORDER[::-1][:-1]:
            zz = (z + d) % Z
            send(part.at[m, rows(zz)], rsb.at[m, z], p_ss.at[m], p_rs.at[m], at(s, zz, j))

    def finish(m):
        total = x[m, j, rows(z), :].astype(F32) + part[m, rows(z), :].astype(F32)
        drain(rsb.at[m, pl.ds(0, Z - 1)], p_rs.at[m])
        for d in range(1, Z):
            total += rsb[m, (z + d) % Z].astype(F32)

        @pl.when(s < LAST)
        def _():
            if m == 0:
                pl.semaphore_wait(ahead, 1)
            slab[2 + m] = total.astype(BF)
            spread(slab.at[2 + m], m, s + 1, z_ss.at[m], False)

        @pl.when(s == LAST)
        def _():
            for g in range(G):
                fin[m, g] = total[2 * g:2 * g + 2, :]
            columns = pl.ds(pl.multiple_of(c * WIDE, WIDE), WIDE)

            @pl.when(y < LAST)
            def _():
                for g in range(G):
                    send(fin.at[m, g], out_ref.at[m, :, columns], f_ss.at[m], f_rs.at[m, c], at(y, z, g))

            @pl.when(y == LAST)
            def _():
                out_ref[m, :, columns] = fin[m, j]
                for k in range(1, G):
                    to = other(j, k)
                    send(fin.at[m, to], out_ref.at[m, :, columns], f_ss.at[m], f_rs.at[m, c], at(s, z, to))

    take_rows(0)

    take_groups(0)
    attend(0)
    own_wo.wait()
    drain(wo.at[pl.ds(0, G - 1)], wo_rs)
    project(0)
    take_rows(1)
    finish(0)
    take_groups(1)
    attend(1)
    project(1)
    finish(1)

    drain(wo.at[pl.ds(0, G - 1)], wo_ss)

    @pl.when(jnp.logical_or(s == 1, s == LAST))
    def _():
        drain(wo.at[pl.ds(0, 4)], m_ss)


    @pl.when(s == 0)
    def _():
        drain(ini_s.at[pl.ds(0, G - 1)], ini_ss)
        for m in range(2):
            drain(x.at[m, 0, pl.ds(0, TOKENS - ROWS)], zi_ss.at[m])

    for m in range(2):
        drain(x.at[m, pl.ds(0, 3)], y_ss.at[m])
        drain(x.at[m, pl.ds(0, 4)], d_ss.at[m])
        drain(att.at[m, pl.ds(0, G - 1)], a_ss.at[m])
        drain(rsb.at[m, pl.ds(0, Z - 1)], p_ss.at[m])

        @pl.when(s < LAST)
        def _():
            drain(x.at[m, 0], z_ss.at[m])

        @pl.when(jnp.logical_and(s == LAST, y < LAST))
        def _():
            drain(fin.at[m], f_ss.at[m])

        @pl.when(jnp.logical_and(s == LAST, y == LAST))
        def _():
            drain(fin.at[m, pl.ds(0, G - 1)], f_ss.at[m])

        for k in range(2):
            @pl.when(jnp.logical_not(jnp.logical_and(s == LAST, jnp.logical_and(y == LAST, c == k))))
            def _():
                drain(out_ref.at[m, :, pl.ds(k * WIDE, WIDE)], f_rs.at[m, k])


def per_device(video_tokens, norm_gain, qkv_weight, out_weight):
    vmem = pl.BlockSpec(memory_space=pltpu.VMEM)
    anywhere = pl.BlockSpec(memory_space=pl.ANY)
    dma, regular = pltpu.SemaphoreType.DMA, pltpu.SemaphoreType.REGULAR
    return pl.pallas_call(
        kernel,
        out_shape=pltpu.VMEM((2, 2, 2 * WIDE), F32),
        in_specs=[anywhere] * 4,
        out_specs=vmem,
        scratch_shapes=[
            pltpu.VMEM((2, 2, D), BF),
            pltpu.VMEM((1, D), F32),
            pltpu.VMEM((2, G, TOKENS, WIDE), BF),
            pltpu.VMEM((3 * HEAD, D), BF),
            pltpu.VMEM((G, WIDE, 3 * PAD), BF),
            pltpu.VMEM((G, HEAD, WIDE), BF),
            pltpu.VMEM((2, HEAD, WIDE), BF),
            pltpu.VMEM((2, HEAD, WIDE), BF),
            pltpu.VMEM((2, TOKENS, 3 * PAD), F32),
            pltpu.VMEM((2, TOKENS, 128), F32),
            pltpu.VMEM((2, G, HEAD, TOKENS), BF),
            pltpu.VMEM((2, TOKENS, WIDE), BF),
            pltpu.VMEM((2, Z, ROWS, WIDE), BF),
            pltpu.VMEM((4, ROWS, WIDE), BF),
            pltpu.VMEM((2, G, 2, WIDE), F32),
            pltpu.VMEM((G, 2, 2, WIDE), F32),
            pltpu.VMEM((G, 2, 2, WIDE), F32),
            dma, dma, dma, dma, dma, dma, dma, dma, regular, regular, regular, dma((2,)), dma, dma((2,)),
            dma((2,)), dma((2,)), dma((2, Z)), dma((2,)), dma((2, 2, 2)),
            dma((2, 2)), dma((2,)), dma((2, 4)), dma((2,)), dma((2,)), dma((2,)), dma((2,)),
            dma((2,)), dma((2, 2)),
        ],
        compiler_params=pltpu.CompilerParams(
            collective_id=0, has_side_effects=True, vmem_limit_bytes=56 * 1024 * 1024
        ),
    )(video_tokens, norm_gain, qkv_weight[0].T, out_weight[0])


def solution(mesh):
    return jax.shard_map(
        per_device,
        mesh=mesh,
        in_specs=(
            P(None, "mesh", None),
            P("section", None),
            P("section", None, "mesh"),
            P("section", "mesh", None),
        ),
        out_specs=P(None, "mesh", "section"),
        check_vma=False,
    )
```
